32 devices in a mesh: rep: 4 (over y, z), dp: 8 (over x, core).
Axes of the slice: x: 4, y: 2, z: 2, core: 2. Of those that a mesh axis runs over, the one named last changes fastest.
The devices are a block of a 4x4x8 slice.
Arguments:
- hidden: bfloat16 [2048, 2048], P(('rep', 'dp')), parts along dimension 0
- ckv_cache: bfloat16 [2048, 128, 512], P(('rep', 'dp')), parts along dimension 0
- kr_cache: bfloat16 [2048, 128, 64], P(('rep', 'dp')), parts along dimension 0
- seq_lens: int32 [2048], P(('rep', 'dp')), parts along dimension 0
- expert_ids: int32 [2048, 6], P(('rep', 'dp')), parts along dimension 0
- attn_gain: bfloat16 [2048], replicated
- kv_gain: bfloat16 [512], replicated
- moe_gain: bfloat16 [2048], replicated
- w_q: bfloat16 [2048, 3072], replicated
- w_dkv: bfloat16 [2048, 576], replicated
- w_uk: bfloat16 [16, 128, 512], replicated
- w_uv: bfloat16 [16, 512, 128], replicated
- w_o: bfloat16 [2048, 2048], replicated
- w_router: bfloat16 [2048, 64], replicated
- shared_gate: bfloat16 [2048, 2816], replicated
- shared_up: bfloat16 [2048, 2816], replicated
- shared_down: bfloat16 [2816, 2048], replicated
- expert_gate: bfloat16 [64, 2048, 1408], P('dp')
- expert_up: bfloat16 [64, 2048, 1408], P('dp')
- expert_down: bfloat16 [64, 1408, 2048], P('dp')
Outputs:
- output 1: bfloat16 [2048, 2048], P(('rep', 'dp')), parts along dimension 0
- output 2: bfloat16 [2048, 512], P(('rep', 'dp')), parts along dimension 0
- output 3: bfloat16 [2048, 64], P(('rep', 'dp')), parts along dimension 0
There are 4 independent parts. The reference program is written for one: setup_inputs(seed, part) draws one part's arguments, and reference() takes and returns one part's arrays. A program takes and returns all parts, laid end to end along the dimension named above; an argument that names none is the same for every part.
All inputs are finite; a program needn't handle non-finite values.
Results may differ from the reference program's by a relative error of at most 0.0123843.
Values are sent between devices in bfloat16 or wider.
A program may use at most 768 MiB of HBM per device.

```python
import jax
import jax.numpy as jnp
from jax import lax

DP_SIZE = 8
SEQS_DEV = 64
CACHE_LEN = 128
D_MODEL = 2048
HEADS = 16
NOPE_DIM = 128
ROPE_DIM = 64
V_DIM = 128
KV_LORA = 512
EXPERTS = 64
TOP_K = 6
FF_DIM = 1408
N_SHARED = 2

GROUP_ROWS = DP_SIZE * SEQS_DEV
SLOT_CAP = max(2, (2 * SEQS_DEV * TOP_K) // EXPERTS)
NORM_EPS = 1e-6
ROPE_THETA = 10000.0
SCORE_SCALE = (NOPE_DIM + ROPE_DIM) ** -0.5


def normal_bf16(draw_key, arr_shape, std_scale):
    return (jax.random.normal(draw_key, arr_shape, jnp.float32) * std_scale).astype(jnp.bfloat16)


def draw_gain(draw_key, gain_len):
    return jax.random.uniform(draw_key, (gain_len,), jnp.float32, minval=0.5, maxval=1.5).astype(jnp.bfloat16)


def draw_lengths(len_key):
    base_key, order_key = jax.random.split(len_key)
    base_lens = jax.random.randint(base_key, (GROUP_ROWS,), CACHE_LEN // 8, CACHE_LEN)
    seq_order = jax.random.permutation(order_key, GROUP_ROWS)
    return base_lens.at[seq_order[0]].set(CACHE_LEN - 1).at[seq_order[1]].set(CACHE_LEN // 8).astype(jnp.int32)


def draw_routes(route_key):
    hot_key, dev_key = jax.random.split(route_key)
    hot_expert = jax.random.randint(hot_key, (), 0, EXPERTS)
    choice_col = jnp.arange(TOP_K)

    def one_device(device_key):
        perm_key, rank_key = jax.random.split(device_key)
        other_ids = jax.random.permutation(perm_key, EXPERTS - 1)
        other_ids = other_ids + (other_ids >= hot_expert).astype(other_ids.dtype)
        tok_rank = jax.random.permutation(rank_key, SEQS_DEV)
        cycle_pos = (tok_rank[:, None] * TOP_K + choice_col[None, :]) % (EXPERTS - 1)
        is_hot = (tok_rank[:, None] < SLOT_CAP) & (choice_col[None, :] == 0)
        return jnp.where(is_hot, hot_expert, other_ids[cycle_pos])

    routes = jax.vmap(one_device)(jax.random.split(dev_key, DP_SIZE))
    return routes.reshape(GROUP_ROWS, TOP_K).astype(jnp.int32)


def setup_inputs(seed: int = 0, part: int = 0) -> dict:
    root_key = jax.random.key(seed)
    part_keys = jax.random.split(jax.random.fold_in(root_key, part), 5)
    weight_keys = jax.random.split(root_key, 15)
    return {
        'hidden': normal_bf16(part_keys[0], (GROUP_ROWS, D_MODEL), 1.0),
        'ckv_cache': normal_bf16(part_keys[1], (GROUP_ROWS, CACHE_LEN, KV_LORA), 1.0),
        'kr_cache': normal_bf16(part_keys[2], (GROUP_ROWS, CACHE_LEN, ROPE_DIM), 1.0),
        'seq_lens': draw_lengths(part_keys[3]),
        'expert_ids': draw_routes(part_keys[4]),
        'attn_gain': draw_gain(weight_keys[0], D_MODEL),
        'kv_gain': draw_gain(weight_keys[1], KV_LORA),
        'moe_gain': draw_gain(weight_keys[2], D_MODEL),
        'w_q': normal_bf16(weight_keys[3], (D_MODEL, HEADS * (NOPE_DIM + ROPE_DIM)), D_MODEL ** -0.5),
        'w_dkv': normal_bf16(weight_keys[4], (D_MODEL, KV_LORA + ROPE_DIM), D_MODEL ** -0.5),
        'w_uk': normal_bf16(weight_keys[5], (HEADS, NOPE_DIM, KV_LORA), NOPE_DIM ** -0.5),
        'w_uv': normal_bf16(weight_keys[6], (HEADS, KV_LORA, V_DIM), 2.0 * KV_LORA ** -0.5),
        'w_o': normal_bf16(weight_keys[7], (HEADS * V_DIM, D_MODEL), 2.0 * (HEADS * V_DIM) ** -0.5),
        'w_router': normal_bf16(weight_keys[8], (D_MODEL, EXPERTS), D_MODEL ** -0.5),
        'shared_gate': normal_bf16(weight_keys[9], (D_MODEL, N_SHARED * FF_DIM), D_MODEL ** -0.5),
        'shared_up': normal_bf16(weight_keys[10], (D_MODEL, N_SHARED * FF_DIM), D_MODEL ** -0.5),
        'shared_down': normal_bf16(weight_keys[11], (N_SHARED * FF_DIM, D_MODEL), (N_SHARED * FF_DIM) ** -0.5),
        'expert_gate': normal_bf16(weight_keys[12], (EXPERTS, D_MODEL, FF_DIM), D_MODEL ** -0.5),
        'expert_up': normal_bf16(weight_keys[13], (EXPERTS, D_MODEL, FF_DIM), D_MODEL ** -0.5),
        'expert_down': normal_bf16(weight_keys[14], (EXPERTS, FF_DIM, D_MODEL), 2.0 * EXPERTS / TOP_K * FF_DIM ** -0.5),
    }


def rms_norm(values, gain_vec):
    vals_f32 = values.astype(jnp.float32)
    inv_rms = lax.rsqrt(jnp.mean(vals_f32 * vals_f32, axis=-1, keepdims=True) + NORM_EPS)
    return (vals_f32 * inv_rms * gain_vec.astype(jnp.float32)).astype(jnp.bfloat16)


def rope_tables(positions):
    inv_freq = ROPE_THETA ** (-2.0 * jnp.arange(ROPE_DIM // 2, dtype=jnp.float32) / ROPE_DIM)
    angles = positions.astype(jnp.float32)[:, None] * inv_freq[None, :]
    return jnp.cos(angles), jnp.sin(angles)


def apply_rope(values, rope_cos, rope_sin):
    half_dim = values.shape[-1] // 2
    first_half = values[..., :half_dim]
    second_half = values[..., half_dim:]
    return jnp.concatenate([first_half * rope_cos - second_half * rope_sin, second_half * rope_cos + first_half * rope_sin], axis=-1)


def attend_one(row_args):
    q_lat_row, q_rot_row, ckv_row, kr_row, seq_len, ckv_new_row, kr_new_row = row_args
    q_lat_f32 = q_lat_row.astype(jnp.float32)
    q_rot_f32 = q_rot_row.astype(jnp.float32)
    ckv_f32 = ckv_row.astype(jnp.float32)
    kr_f32 = kr_row.astype(jnp.float32)
    ckv_new_f32 = ckv_new_row.astype(jnp.float32)
    kr_new_f32 = kr_new_row.astype(jnp.float32)
    scores = (jnp.dot(q_lat_f32, ckv_f32.T) + jnp.dot(q_rot_f32, kr_f32.T)) * SCORE_SCALE
    valid_mask = jnp.arange(CACHE_LEN) < seq_len
    scores = jnp.where(valid_mask[None, :], scores, -jnp.inf)
    new_score = (jnp.dot(q_lat_f32, ckv_new_f32) + jnp.dot(q_rot_f32, kr_new_f32)) * SCORE_SCALE
    top_score = jnp.maximum(jnp.max(scores, axis=-1), new_score)
    exp_cache = jnp.exp(scores - top_score[:, None])
    exp_new = jnp.exp(new_score - top_score)
    denominator = jnp.sum(exp_cache, axis=-1) + exp_new
    prob_cache = (exp_cache / denominator[:, None]).astype(jnp.bfloat16).astype(jnp.float32)
    prob_new = (exp_new / denominator).astype(jnp.bfloat16).astype(jnp.float32)
    o_lat = jnp.dot(prob_cache, ckv_f32) + prob_new[:, None] * ckv_new_f32[None, :]
    return o_lat.astype(jnp.bfloat16)


def routed_experts(moe_in, gate_vals, expert_ids, expert_gate, expert_up, expert_down):
    rows_max = DP_SIZE * SLOT_CAP
    pad_in = jnp.concatenate([moe_in, jnp.zeros((1, D_MODEL), moe_in.dtype)], axis=0)

    def per_expert(acc_out, expert_no):
        picked = expert_ids == expert_no
        gate_tok = jnp.concatenate([jnp.sum(jnp.where(picked, gate_vals, 0.0), axis=-1), jnp.zeros((1,), gate_vals.dtype)])
        row_ids = jnp.nonzero(jnp.any(picked, axis=-1), size=rows_max, fill_value=GROUP_ROWS)[0]
        tok_rows = pad_in[row_ids]
        gate_act = jnp.dot(tok_rows, expert_gate[expert_no], preferred_element_type=jnp.float32)
        up_act = jnp.dot(tok_rows, expert_up[expert_no], preferred_element_type=jnp.float32)
        mid_act = (jax.nn.silu(gate_act) * up_act).astype(jnp.bfloat16)
        expert_out = jnp.dot(mid_act, expert_down[expert_no], preferred_element_type=jnp.float32).astype(jnp.bfloat16)
        acc_out = acc_out.at[row_ids].add(gate_tok[row_ids][:, None] * expert_out.astype(jnp.float32), mode='drop')
        return acc_out, None

    scanned = lax.scan(per_expert, jnp.zeros((GROUP_ROWS, D_MODEL), jnp.float32), jnp.arange(EXPERTS))
    return scanned[0]


def reference(hidden, ckv_cache, kr_cache, seq_lens, expert_ids, attn_gain, kv_gain, moe_gain, w_q, w_dkv, w_uk, w_uv, w_o, w_router, shared_gate, shared_up, shared_down, expert_gate, expert_up, expert_down):
    normed_x = rms_norm(hidden, attn_gain)
    q_all = jnp.dot(normed_x, w_q, preferred_element_type=jnp.float32).astype(jnp.bfloat16).reshape(GROUP_ROWS, HEADS, NOPE_DIM + ROPE_DIM)
    latent_kv = jnp.dot(normed_x, w_dkv, preferred_element_type=jnp.float32)
    ckv_new = rms_norm(latent_kv[:, :KV_LORA], kv_gain)
    rope_cos, rope_sin = rope_tables(seq_lens)
    kr_new = apply_rope(latent_kv[:, KV_LORA:], rope_cos, rope_sin).astype(jnp.bfloat16)
    q_rot = apply_rope(q_all[:, :, NOPE_DIM:].astype(jnp.float32), rope_cos[:, None, :], rope_sin[:, None, :]).astype(jnp.bfloat16)
    q_lat = jnp.einsum('bhn,hnc->bhc', q_all[:, :, :NOPE_DIM].astype(jnp.float32), w_uk.astype(jnp.float32)).astype(jnp.bfloat16)
    o_lat = lax.map(attend_one, (q_lat, q_rot, ckv_cache, kr_cache, seq_lens, ckv_new, kr_new))
    head_out = jnp.einsum('bhc,hcv->bhv', o_lat.astype(jnp.float32), w_uv.astype(jnp.float32)).astype(jnp.bfloat16).reshape(GROUP_ROWS, HEADS * V_DIM)
    resid_out = (hidden.astype(jnp.float32) + jnp.dot(head_out, w_o, preferred_element_type=jnp.float32)).astype(jnp.bfloat16)
    moe_in = rms_norm(resid_out, moe_gain)
    router_prob = jax.nn.softmax(jnp.dot(moe_in, w_router, preferred_element_type=jnp.float32), axis=-1)
    gate_vals = jnp.take_along_axis(router_prob, expert_ids, axis=-1)
    shared_act = (jax.nn.silu(jnp.dot(moe_in, shared_gate, preferred_element_type=jnp.float32)) * jnp.dot(moe_in, shared_up, preferred_element_type=jnp.float32)).astype(jnp.bfloat16)
    shared_out = jnp.dot(shared_act, shared_down, preferred_element_type=jnp.float32)
    routed_out = routed_experts(moe_in, gate_vals, expert_ids, expert_gate, expert_up, expert_down)
    layer_out = (resid_out.astype(jnp.float32) + shared_out + routed_out).astype(jnp.bfloat16)
    return layer_out, ckv_new, kr_new
```

```python
import functools

import jax
import jax.numpy as jnp
from jax import lax
from jax.experimental import pallas as pl
from jax.experimental.pallas import tpu as pltpu
from jax.sharding import PartitionSpec as P

NORM_EPS = 1e-6
ROPE_THETA = 10000.0
MESH = pl.DeviceIdType.MESH
MAIN = 8
CODE = 16


def dot_f32(lhs, rhs):
    return jnp.dot(lhs, rhs, preferred_element_type=jnp.float32)


def iota2(shape, dim):
    return lax.broadcasted_iota(jnp.int32, shape, dim)


def div_const(vals, num):
    return ((vals.astype(jnp.float32) + 0.5) * (1.0 / num)).astype(jnp.int32)


def gate_up(rows, gate_ref, up_ref, mid_ref):
    ff_dim = gate_ref.shape[1]
    for col in range(0, ff_dim, 512):
        cols = pl.ds(col, min(512, ff_dim - col))
        gate_act = dot_f32(rows[...], gate_ref[:, cols])
        up_act = dot_f32(rows[...], up_ref[:, cols])
        mid_ref[:, cols] = (jax.nn.silu(gate_act) * up_act).astype(jnp.bfloat16)


def row_of(vec_ref):
    vals = vec_ref[...].astype(jnp.float32)
    return jnp.concatenate([vals[i : i + 1, :] for i in range(vals.shape[0])], axis=1)


def column_of(row, size):
    same = iota2((size, size), 0) == iota2((size, size), 1)
    return jnp.sum(jnp.where(same, row, 0), axis=1, keepdims=True)


def dot_t(lhs, rhs):
    return lax.dot_general(lhs, rhs, (((1,), (1,)), ((), ())), preferred_element_type=jnp.float32)


def rounded(vals):
    return vals.astype(jnp.bfloat16).astype(jnp.float32)


def layer_kernel(
    group,
    cap,
    nope_dim,
    hidden,
    ckv_cache,
    kr_cache_t,
    lens_hbm,
    ids_hbm,
    attn_gain,
    kv_gain,
    moe_gain,
    w_q,
    w_dkv_t,
    w_uk,
    w_uv,
    w_o,
    router_t,
    sh_gate,
    sh_up,
    sh_down,
    ex_gate,
    ex_up,
    ex_down,
    out_ref,
    ckv_new_ref,
    kr_new_ref,
    hid,
    lens_v,
    ids_v,
    attn_g,
    kv_g,
    moe_g,
    router_v,
    ckv,
    krt,
    q_scr,
    q_lat,
    q_rot,
    o_lat,
    c_new,
    k_new,
    len_rows,
    heads_out,
    resid_v,
    u_all,
    codes,
    gate_buf,
    up_buf,
    down_buf,
    pick,
    rows,
    mid,
    mid_sh,
    stage,
    y_buf,
    back,
    w_sel,
    perm,
    s_acc,
    r_acc,
    small_sem,
    a_sem,
    ckv_sem,
    w_sem,
    u_send,
    u_recv,
    p_send,
    p_recv,
    c_send,
    c_recv,
    y_send,
    y_recv,
    own_sem,
):
    me = lax.axis_index('dp')
    toks, width = hidden.shape
    top_k = ids_hbm.shape[0]
    local = ex_gate.shape[0]
    experts = local * group
    ff_dim = ex_gate.shape[2]
    pairs = local // 2
    slots = group * cap
    chip, core = me // 2, lax.rem(me, 2)
    chips = group // 2
    cache_len, lora = ckv_cache.shape[1:]
    rope_dim = kr_cache_t.shape[1]
    head_dim = nope_dim + rope_dim
    heads = w_q.shape[1] // head_dim
    scale = head_dim**-0.5
    q_rest = w_q.shape[1] - 2 * ff_dim
    uk_col = q_rest
    uv_col = uk_col + lora
    o_rest = w_o.shape[0] - ff_dim
    dkv_dim = w_dkv_t.shape[0]
    v_dim = w_uv.shape[2]
    per_col = width // lora

    bufs = (gate_buf, up_buf, down_buf)

    def shared_copy(half, slot, which):
        part = pl.ds(half * ff_dim, ff_dim)
        src = (sh_gate, sh_up)[which].at[:, part] if which < 2 else sh_down.at[part, :]
        return pltpu.make_async_copy(src, bufs[which].at[slot], w_sem.at[which, slot])

    def expert_copy(idx, slot, which):
        return pltpu.make_async_copy((ex_gate, ex_up, ex_down)[which].at[idx], bufs[which].at[slot], w_sem.at[which, slot])

    seqs = 8

    def ckv_copy(part):
        block = pl.ds(pl.multiple_of(part * seqs, seqs), seqs)
        return pltpu.make_async_copy(ckv_cache.at[block], ckv.at[block], ckv_sem.at[part])

    smalls = [
        (hidden, hid), (attn_gain, attn_g), (kv_gain, kv_g), (moe_gain, moe_g), (lens_hbm, lens_v), (ids_hbm, ids_v), (router_t, router_v)]
    small = [functools.partial(pltpu.make_async_copy, src, dst, small_sem.at[i]) for i, (src, dst) in enumerate(smalls)]
    attn = [
        (w_q.at[:, pl.ds(0, ff_dim)], gate_buf.at[0]),
        (w_q.at[:, pl.ds(ff_dim, ff_dim)], up_buf.at[0]),
        (w_q.at[:, pl.ds(2 * ff_dim, q_rest)], gate_buf.at[1, :, pl.ds(0, q_rest)]),
        (w_dkv_t, down_buf.at[0, pl.ds(0, dkv_dim), :]),
        (w_uk, gate_buf.at[1, :, pl.ds(uk_col, lora)]),
        (kr_cache_t, krt),
        (w_o.at[pl.ds(0, ff_dim), :], down_buf.at[1]),
        (w_o.at[pl.ds(ff_dim, o_rest), :], down_buf.at[0, pl.ds(dkv_dim, o_rest), :]),
    ]
    for col in range(heads // per_col):
        attn.append((w_uv.at[col], gate_buf.at[1, :, pl.ds(uv_col + col * v_dim, v_dim)]))
    attn = [functools.partial(pltpu.make_async_copy, src, dst, a_sem.at[i]) for i, (src, dst) in enumerate(attn)]
    for make in small:
        make().start()
    for make in attn[:6]:
        make().start(priority=1)
    for part in range(toks // seqs):
        ckv_copy(part).start(priority=1)
    for make in attn[8:] + attn[6:8]:
        make().start(priority=1)
    shared_copy(1, 1, 1).start(priority=1)
    barrier = pltpu.get_barrier_semaphore()
    for step in range(1, group):
        pl.semaphore_signal(barrier, inc=1, device_id={'dp': lax.rem(me + step, group)}, device_id_type=MESH)

    small[0]().wait()
    small[1]().wait()
    hid_f = hid[...].astype(jnp.float32)
    inv_rms = lax.rsqrt(jnp.mean(hid_f * hid_f, axis=-1, keepdims=True) + NORM_EPS)
    normed = (hid_f * inv_rms * row_of(attn_g)).astype(jnp.bfloat16)
    attn[0]().wait()
    for col in range(0, ff_dim, 512):
        cols = pl.ds(col, min(512, ff_dim - col))
        q_scr[:, cols] = rounded(dot_f32(normed, gate_buf[0, :, cols]))
    shared_copy(0, 0, 0).start(priority=1)
    attn[1]().wait()
    for col in range(0, ff_dim, 512):
        size = min(512, ff_dim - col)
        q_scr[:, pl.ds(ff_dim + col, size)] = rounded(dot_f32(normed, up_buf[0, :, pl.ds(col, size)]))
    shared_copy(0, 0, 1).start(priority=1)
    attn[2]().wait()
    q_scr[:, pl.ds(2 * ff_dim, q_rest)] = rounded(dot_f32(normed, gate_buf[1, :, pl.ds(0, q_rest)]))
    for make in small[2:]:
        make().wait()
    lens_row = lens_v[...]
    lens_col = column_of(lens_row, toks)
    len_rows[...] = jnp.broadcast_to(lens_col, len_rows.shape)
    lane1 = iota2((1, 128), 1)
    freq_no = lax.rem(lane1, rope_dim // 2)
    freqs = jnp.zeros((1, 128), jnp.float32)
    for i in range(rope_dim // 2):
        freqs = jnp.where(freq_no == i, ROPE_THETA ** (-2.0 * i / rope_dim), freqs)
    angles = lens_col.astype(jnp.float32) * freqs
    rope_cos = jnp.cos(angles)
    rope_sin = jnp.sin(angles)
    lane_t = iota2((toks, 128), 1)
    first_half = lax.rem(lane_t, rope_dim) < rope_dim // 2
    low_half = lane_t < rope_dim
    rope_sin = jnp.where(first_half, -rope_sin, rope_sin)

    def rope(vals):
        ahead = pltpu.roll(vals, 128 - rope_dim // 2, 1)
        behind = pltpu.roll(vals, rope_dim // 2, 1)
        return vals * rope_cos + jnp.where(first_half, ahead, behind) * rope_sin

    attn[3]().wait()
    latent = dot_t(normed, down_buf[0, pl.ds(0, dkv_dim), :])
    c_part = latent[:, :lora]
    c_rms = lax.rsqrt(jnp.mean(c_part * c_part, axis=-1, keepdims=True) + NORM_EPS)
    c_row = (c_part * c_rms * row_of(kv_g)).astype(jnp.bfloat16)
    ckv_new_ref[...] = c_row
    c_new[...] = c_row.astype(jnp.float32)
    k_part = jnp.concatenate([latent[:, lora:], latent[:, lora:]], axis=1)
    k_row = rope(k_part).astype(jnp.bfloat16)
    kr_new_ref[...] = k_row[:, :rope_dim]
    k_new[...] = k_row.astype(jnp.float32)

    attn[4]().wait()
    for m in range(heads // 2):
        q_a = q_scr[:, pl.ds(2 * m * head_dim, 128)]
        q_b = q_scr[:, pl.ds(2 * m * head_dim + 128, 128)]
        q_c = q_scr[:, pl.ds(2 * m * head_dim + 256, 128)]
        swap_b, swap_c = pltpu.roll(q_b, 64, 1), pltpu.roll(q_c, 64, 1)
        nope = (q_a, jnp.where(low_half, swap_b, swap_c))
        rot = rope(jnp.where(low_half, q_b, q_c))
        rot = (rounded(rot), rounded(pltpu.roll(rot, 64, 1)))
        for i in range(2):
            head = 2 * m + i
            lat = dot_f32(nope[i].astype(jnp.bfloat16), gate_buf[1, pl.ds(head * nope_dim, nope_dim), pl.ds(uk_col, lora)])
            for c in range(lora // 128):
                q_lat[c, pl.ds(head, toks, stride=heads), :] = rounded(lat[:, c * 128 : c * 128 + 128])
            q_rot[pl.ds(head, toks, stride=heads), :] = jnp.where(low_half, rot[i], 0.0)

    attn[5]().wait()
    key_no = iota2((heads, cache_len), 1)

    def attend(part, carry):
        ckv_copy(part).wait()
        found = []
        for i in range(seqs):
            seq = part * seqs + i
            block = pl.ds(pl.multiple_of(seq * heads, heads), heads)
            lat = jnp.concatenate([q_lat[c, block, :] for c in range(lora // 128)], axis=1)
            rot = q_rot[block, :]
            c_one, k_one = c_new[pl.ds(seq, 1), :], k_new[pl.ds(seq, 1), :]
            score = dot_t(lat.astype(jnp.bfloat16), ckv[seq]) + dot_f32(rot[:, :rope_dim].astype(jnp.bfloat16), krt[seq])
            new = jnp.sum(lat * c_one, axis=-1, keepdims=True) + jnp.sum(rot * k_one, axis=-1, keepdims=True)
            score = jnp.where(key_no < len_rows[pl.ds(seq, 1), :], score * scale, -jnp.inf)
            found.append((seq, block, c_one, score, new * scale))
        weights = []
        for seq, block, c_one, score, new in found:
            top = jnp.maximum(jnp.max(score, axis=-1, keepdims=True), new)
            exp_c, exp_n = jnp.exp(score - top), jnp.exp(new - top)
            total = jnp.sum(exp_c, axis=-1, keepdims=True) + exp_n
            weights.append(((exp_c / total).astype(jnp.bfloat16), rounded(exp_n / total)))
        for (seq, block, c_one, _, _), (prob, prob_new) in zip(found, weights):
            lat = rounded(dot_f32(prob, ckv[seq]) + prob_new * c_one)
            for c in range(lora // 128):
                o_lat[c, block, :] = lat[:, c * 128 : c * 128 + 128]
        return carry

    lax.fori_loop(0, toks // seqs, attend, 0)

    for make in attn[8:]:
        make().wait()
    for head in range(heads):
        o_head = jnp.concatenate([o_lat[c, pl.ds(head, toks, stride=heads), :] for c in range(lora // 128)], axis=1).astype(jnp.bfloat16)
        w_head = gate_buf[1, pl.ds(head % per_col * lora, lora), pl.ds(uv_col + head // per_col * v_dim, v_dim)]
        heads_out[:, pl.ds(head * v_dim, v_dim)] = dot_f32(o_head, w_head).astype(jnp.bfloat16)
    shared_copy(1, 1, 0).start(priority=1)
    attn[6]().wait()
    attn[7]().wait()
    for col in range(0, width, 512):
        cols = pl.ds(col, 512)
        part = dot_f32(heads_out[:, pl.ds(0, ff_dim)], down_buf[1, :, cols])
        part += dot_f32(heads_out[:, pl.ds(ff_dim, o_rest)], down_buf[0, pl.ds(dkv_dim, o_rest), cols])
        resid_v[:, cols] = (hid[:, cols].astype(jnp.float32) + part).astype(jnp.bfloat16)
    shared_copy(0, 0, 2).start(priority=1)
    expert_copy(0, 1, 2).start(priority=1)

    resid = resid_v[...].astype(jnp.float32)
    inv_rms = lax.rsqrt(jnp.mean(resid * resid, axis=-1, keepdims=True) + NORM_EPS)
    moe_in = (resid * inv_rms * row_of(moe_g)).astype(jnp.bfloat16)
    mine = pl.ds(pl.multiple_of(me * toks, toks), toks)
    u_all[mine, :] = moe_in

    ids_t = jnp.concatenate([ids_v[...], ids_v[...]], axis=1)
    lanes = ids_t.shape[1]
    exp_row = iota2((experts, lanes), 0)
    picked_t = jnp.zeros((experts, lanes), jnp.float32)
    for k in range(top_k):
        picked_t += jnp.where(ids_t[k : k + 1, :] == exp_row, 1.0, 0.0)
    from_t, to_t = iota2((lanes, lanes), 0), iota2((lanes, lanes), 1)
    before = (from_t < to_t) & ((from_t < toks) == (to_t < toks))
    rank_t = dot_f32(picked_t.astype(jnp.bfloat16), jnp.where(before, 1.0, 0.0).astype(jnp.bfloat16))
    code_t = jnp.full((8, lanes), -1, jnp.int32)
    for k in range(top_k):
        rank_k = jnp.sum(jnp.where(ids_t[k : k + 1, :] == exp_row, rank_t, 0.0), axis=0, keepdims=True)
        code_k = ids_t[k : k + 1, :] * CODE + rank_k.astype(jnp.int32)
        code_t = jnp.where(iota2((8, lanes), 0) == k, code_k, code_t)
    codes[me] = code_t

    pl.semaphore_wait(barrier, group - 1)

    def code_copy(step):
        return pltpu.make_async_remote_copy(
            src_ref=codes.at[me], dst_ref=codes.at[me], send_sem=c_send.at[step], recv_sem=c_recv.at[step],
            device_id={'dp': lax.rem(me + step, group)}, device_id_type=MESH)

    def rows_at(dev, first, size):
        return u_all.at[pl.ds(pl.multiple_of(dev * toks + first, 8), size), :]

    hops = (1, chips - 1)
    half = toks // 2

    def piece(way, turn):
        back_by = hops[way] if turn < 2 else 2 * hops[way]
        part = (way + turn) % 2
        return rows_at(lax.rem(chip + 2 * chips - back_by, chips) * 2 + core, part * half, half)

    def ring_copy(way, turn):
        block = piece(way, 0) if turn == 2 else rows_at(me, (way + turn) % 2 * half, half)
        return pltpu.make_async_remote_copy(
            src_ref=block, dst_ref=block, send_sem=u_send.at[way, turn], recv_sem=u_recv.at[way, turn],
            device_id={'dp': lax.rem(chip + hops[way], chips) * 2 + core}, device_id_type=MESH)

    def partner_copy(way, turn):
        block = rows_at(me, 0, toks) if way == 2 else piece(way, turn)
        return pltpu.make_async_remote_copy(
            src_ref=block, dst_ref=block, send_sem=p_send.at[way, turn], recv_sem=p_recv.at[way, turn],
            device_id={'dp': chip * 2 + 1 - core}, device_id_type=MESH)

    for turn in range(2):
        for way in range(2):
            ring_copy(way, turn).start()
    partner_copy(2, 0).start()
    for step in range(1, group):
        code_copy(step).start()

    logits = dot_t(moe_in, router_v[...])
    exp_l = jnp.exp(logits - jnp.max(logits, axis=-1, keepdims=True))
    probs = exp_l / jnp.sum(exp_l, axis=-1, keepdims=True)
    ids = [column_of(ids_v[k : k + 1, :], toks) for k in range(top_k)]
    exp_col = iota2((toks, experts), 1)
    picked = jnp.zeros((toks, experts), jnp.float32)
    for k in range(top_k):
        picked += jnp.where(ids[k] == exp_col, 1.0, 0.0)
    earlier = jnp.where(iota2((toks, toks), 1) < iota2((toks, toks), 0), 1.0, 0.0).astype(jnp.bfloat16)
    rank = dot_f32(earlier, picked.astype(jnp.bfloat16))
    gates, tok_codes = [], []
    for k in range(top_k):
        hit = ids[k] == exp_col
        gates.append(jnp.sum(jnp.where(hit, probs, 0.0), axis=-1, keepdims=True))
        rank_k = jnp.sum(jnp.where(hit, rank, 0.0), axis=-1, keepdims=True)
        tok_codes.append(ids[k] * CODE + rank_k.astype(jnp.int32))
    lane = iota2((toks, 2 * slots), 1)
    sec = div_const(lane, group * MAIN)
    owner = div_const(lane - sec * group * MAIN, MAIN)
    spot = lane - sec * group * MAIN - owner * MAIN
    second = jnp.where(sec == 2, jnp.where(spot >= cap - MAIN, 1, 0), sec)
    spot = jnp.where(sec == 2, MAIN + spot - second * (cap - MAIN), spot)
    base = (owner * local + second) * CODE + spot
    for pair in range(pairs):
        slot_code = base + 2 * pair * CODE
        gate_sel = jnp.zeros((toks, 2 * slots), jnp.float32)
        for k in range(top_k):
            gate_sel += jnp.where(tok_codes[k] == slot_code, gates[k], 0.0)
        high = gate_sel.astype(jnp.bfloat16)
        rest = gate_sel - high.astype(jnp.float32)
        middle = rest.astype(jnp.bfloat16)
        low = (rest - middle.astype(jnp.float32)).astype(jnp.bfloat16)
        w_sel[pair, pl.ds(0, toks), :] = high
        w_sel[pair, pl.ds(toks, toks), :] = middle
        w_sel[pair, pl.ds(2 * toks, toks), :] = low
    extra = group * MAIN
    out_row = iota2((extra, extra), 0)
    dev_row = div_const(out_row, MAIN)
    spot = out_row - dev_row * MAIN
    second = jnp.where(spot >= cap - MAIN, 1, 0)
    from_row = second * (slots - extra) + dev_row * (cap - MAIN) + spot - second * (cap - MAIN)
    perm[...] = jnp.where(from_row == iota2((extra, extra), 1), 1.0, 0.0).astype(jnp.bfloat16)

    def shared_down(slot):
        for col in range(0, width, 512):
            yield pl.ds(col, 512), dot_f32(mid_sh[...], down_buf[slot, :, pl.ds(col, 512)])

    shared_copy(0, 0, 0).wait()
    shared_copy(0, 0, 1).wait()
    gate_up(u_all.at[mine, :], gate_buf.at[0], up_buf.at[0], mid_sh)
    expert_copy(0, 0, 0).start(priority=1)
    expert_copy(0, 0, 1).start(priority=1)
    shared_copy(0, 0, 2).wait()
    for cols, part in shared_down(0):
        s_acc[:, cols] = part
    expert_copy(1, 0, 2).start(priority=1)
    for way in range(2):
        ring_copy(way, 0).wait_recv()
        ring_copy(way, 2).start()
        partner_copy(way, 0).start()
    shared_copy(1, 1, 0).wait()
    shared_copy(1, 1, 1).wait()
    gate_up(u_all.at[mine, :], gate_buf.at[1], up_buf.at[1], mid_sh)
    expert_copy(1, 1, 0).start(priority=1)
    expert_copy(1, 1, 1).start(priority=1)

    for turn in range(1, 3):
        for way in range(2):
            ring_copy(way, turn).wait_recv()
            partner_copy(way, turn).start()
    for step in range(1, group):
        code_copy(step).wait_recv()
    partner_copy(2, 0).wait_recv()
    for turn in range(3):
        for way in range(2):
            partner_copy(way, turn).wait_recv()

    row = iota2((slots, lanes), 0)
    late = row >= extra
    row_dev = jnp.where(late, div_const(row - extra, cap - MAIN), div_const(row, MAIN))
    row_rank = jnp.where(late, MAIN + row - extra - row_dev * (cap - MAIN), row - row_dev * MAIN)
    lane_odd = jnp.where(iota2((slots, lanes), 1) >= toks, 1, 0)
    tile_odd = iota2((8, lanes), 1) >= toks

    def slot_block(pair, sec, dev):
        return pair, pl.ds(pl.multiple_of(sec * extra + dev * MAIN, MAIN), MAIN)

    def y_copy(pair, sec, step):
        dev = lax.rem(me + step, group)
        return pltpu.make_async_remote_copy(
            src_ref=y_buf.at[slot_block(pair, sec, dev)], dst_ref=back.at[slot_block(pair, sec, me)],
            send_sem=y_send.at[pair, sec, step], recv_sem=y_recv.at[pair, sec, step],
            device_id={'dp': dev}, device_id_type=MESH)

    def own_copy(pair, sec):
        return pltpu.make_async_copy(y_buf.at[slot_block(pair, sec, me)], back.at[slot_block(pair, sec, me)], own_sem.at[pair, sec])

    def send_back(pair, sec):
        for step in (4, 3, 5, 2, 6, 7, 1):
            y_copy(pair, sec, step).start()
        own_copy(pair, sec).start()

    def expert_step(idx, carry):
        slot = lax.rem(idx, 2)
        slot_d = 1 - slot
        target = (me * local + idx) * CODE + row_rank
        for chunk in range(group // 2):
            code_c = jnp.where(tile_odd, codes[2 * chunk + 1], codes[2 * chunk])
            hit = code_c[0:1, :] == target
            for k in range(1, top_k):
                hit = hit | (code_c[k : k + 1, :] == target)
            hit = hit & (row_dev == 2 * chunk + lane_odd)
            pick[:, pl.ds(chunk * lanes, lanes)] = jnp.where(hit, 1.0, 0.0).astype(jnp.bfloat16)
        for col in range(0, width, 512):
            rows[:, pl.ds(col, 512)] = dot_f32(pick[...], u_all[:, pl.ds(col, 512)]).astype(jnp.bfloat16)
        expert_copy(idx, slot, 0).wait()
        expert_copy(idx, slot, 1).wait()
        gate_up(rows, gate_buf.at[slot], up_buf.at[slot], mid)

        @pl.when(idx < local - 2)
        def _():
            expert_copy(idx + 2, slot, 0).start(priority=1)
            expert_copy(idx + 2, slot, 1).start(priority=1)

        expert_copy(idx, slot_d, 2).wait()
        for col in range(0, width, 512):
            cols = pl.ds(col, 512)
            expert_out = dot_f32(mid[...], down_buf[slot_d, :, cols]).astype(jnp.bfloat16)
            y_buf[idx // 2, pl.ds(pl.multiple_of(slot * extra, 8), extra), cols] = expert_out[:extra]
            stage[pl.ds(pl.multiple_of(slot * (slots - extra), 8), slots - extra), cols] = expert_out[extra:]

        @pl.when(idx < local - 2)
        def _():
            expert_copy(idx + 2, slot_d, 2).start(priority=1)

        @pl.when(idx == local - 2)
        def _():
            shared_copy(1, slot_d, 2).start(priority=1)

        send_back(idx // 2, slot)

        @pl.when(slot == 1)
        def _():
            pair = idx // 2
            for col in range(0, width, 512):
                cols = pl.ds(col, 512)
                y_buf[pair, pl.ds(2 * extra, extra), cols] = dot_f32(perm[...], stage[:, cols]).astype(jnp.bfloat16)
            send_back(pair, 2)

        return carry

    lax.fori_loop(0, local, expert_step, 0)

    last = (local + 1) % 2
    shared_copy(1, last, 2).wait()
    for cols, part in shared_down(last):
        s_acc[:, cols] += part

    for pair in range(pairs):
        for sec in range(3):
            for step in range(1, group):
                y_copy(pair, sec, step).wait_recv()
            own_copy(pair, sec).wait()
        for col in range(0, width, 512):
            cols = pl.ds(col, 512)
            part = dot_f32(w_sel[pair], back[pair, :, cols])
            part = part[0:toks] + part[toks : 2 * toks] + part[2 * toks :]
            if pair == 0:
                r_acc[:, cols] = part
            else:
                r_acc[:, cols] += part
    out_ref[...] = (resid_v[...].astype(jnp.float32) + s_acc[...] + r_acc[...]).astype(jnp.bfloat16)

    for step in range(1, group):
        code_copy(step).wait_send()
    partner_copy(2, 0).wait_send()
    for turn in range(3):
        for way in range(2):
            ring_copy(way, turn).wait_send()
            partner_copy(way, turn).wait_send()
    for pair in range(pairs):
        for sec in range(3):
            for step in range(1, group):
                y_copy(pair, sec, step).wait_send()


def store_kernel(*refs):
    sems = refs[-1]
    copies = [pltpu.make_async_copy(refs[i], refs[i + 3], sems.at[i]) for i in range(3)]
    for copy in copies:
        copy.start()
    for copy in copies:
        copy.wait()


def solution(mesh):
    row_spec = P(('rep', 'dp'))
    full_spec = P()
    expert_spec = P('dp')
    group = mesh.shape['dp']

    def device_step(hidden, ckv_cache, kr_cache, seq_lens, expert_ids, attn_gain, kv_gain, moe_gain, w_q, w_dkv, w_uk, w_uv, w_o, w_router, shared_gate, shared_up, shared_down, expert_gate, expert_up, expert_down):
        toks, width = hidden.shape
        top_k = expert_ids.shape[1]
        experts = w_router.shape[1]
        local, _, ff_dim = expert_gate.shape
        heads, nope_dim, lora = w_uk.shape
        v_dim = w_uv.shape[2]
        cache_len, rope_dim = kr_cache.shape[1:]
        cap = max(2, 2 * toks * top_k // experts)
        slots = group * cap
        pairs = local // 2
        hbm = pl.BlockSpec(memory_space=pltpu.HBM)
        vmem = pl.BlockSpec(memory_space=pltpu.VMEM)
        dma = pltpu.SemaphoreType.DMA
        bf16, f32, i32 = jnp.bfloat16, jnp.float32, jnp.int32
        operands = (
            hidden, ckv_cache, kr_cache.transpose(0, 2, 1), seq_lens.reshape(1, toks), expert_ids.T,
            attn_gain.reshape(-1, 128), kv_gain.reshape(-1, 128), moe_gain.reshape(-1, 128),
            w_q, w_dkv.T, w_uk.reshape(heads * nope_dim, lora), w_uv.reshape(-1, width, v_dim), w_o, w_router.T,
            shared_gate, shared_up, shared_down, expert_gate, expert_up, expert_down)
        scratch = [
            ((toks, width), bf16), ((1, toks), i32), ((top_k, toks), i32), ((width // 128, 128), bf16), ((lora // 128, 128), bf16),
            ((width // 128, 128), bf16), ((experts, width), bf16), ((toks, cache_len, lora), bf16), ((toks, rope_dim, cache_len), bf16),
            ((toks, w_q.shape[1]), f32), ((lora // 128, toks * heads, 128), f32), ((toks * heads, 128), f32), ((lora // 128, toks * heads, 128), f32),
            ((toks, lora), f32), ((toks, 128), f32), ((toks, 128), i32), ((toks, heads * v_dim), bf16), ((toks, width), bf16),
            ((group * toks, width), bf16), ((group, 8, 2 * toks), i32),
            ((2, width, ff_dim), bf16), ((2, width, ff_dim), bf16), ((2, ff_dim, width), bf16),
            ((slots, group * toks), bf16), ((slots, width), bf16), ((slots, ff_dim), bf16), ((toks, ff_dim), bf16),
            ((2 * (slots - group * MAIN), width), bf16), ((pairs, 2 * slots, width), bf16), ((pairs, 2 * slots, width), bf16),
            ((pairs, 3 * toks, 2 * slots), bf16), ((group * MAIN, group * MAIN), bf16), ((toks, width), f32), ((toks, width), f32)]
        sems = [(7,), (8 + heads * lora // width,), (toks // 8,), (3, 2), (2, 3), (2, 3), (3, 3), (3, 3), (group,), (group,), (pairs, 3, group), (pairs, 3, group), (pairs, 3)]
        results = pl.pallas_call(
            functools.partial(layer_kernel, group, cap, nope_dim),
            out_shape=(pltpu.VMEM((toks, width), bf16), pltpu.VMEM((toks, lora), bf16), pltpu.VMEM((toks, rope_dim), bf16)),
            in_specs=[hbm] * len(operands),
            out_specs=(vmem, vmem, vmem),
            scratch_shapes=[pltpu.VMEM(shape, dtype) for shape, dtype in scratch] + [dma(shape) for shape in sems],
            compiler_params=pltpu.CompilerParams(collective_id=0, has_side_effects=True, vmem_limit_bytes=66 * 10**6),
        )(*operands)
        return pl.pallas_call(
            store_kernel, out_shape=tuple(jax.ShapeDtypeStruct(x.shape, x.dtype) for x in results),
            in_specs=[vmem] * 3, out_specs=(hbm, hbm, hbm), scratch_shapes=[dma((3,))],
            compiler_params=pltpu.CompilerParams(vmem_limit_bytes=2**20),
        )(*results)

    in_specs = (row_spec,) * 5 + (full_spec,) * 12 + (expert_spec,) * 3
    return jax.shard_map(device_step, mesh=mesh, in_specs=in_specs, out_specs=(row_spec, row_spec, row_spec), check_vma=False)
```
